8 devices in a mesh: model: 2 (over z, y), data: 4 (over x, core).
Axes of the slice: x: 2, y: 2, z: 1, core: 2. Of those that a mesh axis runs over, the one named last changes fastest.
Arguments:
- act_in: bfloat16 [32768, 1024], P('data')
- grad_out: bfloat16 [32768, 1024], P('data')
- w_up: bfloat16 [2, 1024, 2816], P(None, None, 'model')
- w_down: bfloat16 [2, 2816, 1024], P(None, 'model')
- master_up: float32 [2, 1024, 2816], P(None, 'data', 'model')
- master_down: float32 [2, 2816, 1024], P(None, ('model', 'data'))
- mom_up: float32 [2, 1024, 2816], P(None, 'data', 'model')
- mom_down: float32 [2, 2816, 1024], P(None, ('model', 'data'))
- var_up: float32 [2, 1024, 2816], P(None, 'data', 'model')
- var_down: float32 [2, 2816, 1024], P(None, ('model', 'data'))
- learn_rate: float32 [1], replicated
- clip_norm: float32 [1], replicated
Outputs:
- output 1: bfloat16 [2, 1024, 2816], P(None, None, 'model')
- output 2: bfloat16 [2, 2816, 1024], P(None, 'model')
- output 3: float32 [2, 1024, 2816], P(None, 'data', 'model')
- output 4: float32 [2, 2816, 1024], P(None, ('model', 'data'))
- output 5: float32 [2, 1024, 2816], P(None, 'data', 'model')
- output 6: float32 [2, 2816, 1024], P(None, ('model', 'data'))
- output 7: float32 [2, 1024, 2816], P(None, 'data', 'model')
- output 8: float32 [2, 2816, 1024], P(None, ('model', 'data'))
- output 9: float32 [1], replicated
All inputs are finite; a program needn't handle non-finite values.
Results may differ from the reference program's by a relative error of at most 0.0014616.
Values are sent between devices in bfloat16 or wider.
A program may use at most 1 GiB of HBM per device.

```python
import jax
import jax.numpy as jnp
from jax import lax

D = 1024
FF = 2816
TOKENS_DEV = 8192
DATA = 4
STEP = 10
ROWS = DATA * TOKENS_DEV

BETA_ONE = 0.9
BETA_TWO = 0.95
ADAM_EPS = 1e-8
NORM_EPS = 1e-6


def matmul(left_op, right_op):
    return jnp.dot(left_op, right_op, preferred_element_type=jnp.float32)


def gelu_fwd(z_low):
    return jax.nn.gelu(z_low.astype(jnp.float32)).astype(jnp.bfloat16)


def gelu_back(z_low, grad_low):
    _, back_fn = jax.vjp(jax.nn.gelu, z_low.astype(jnp.float32))
    return back_fn(grad_low.astype(jnp.float32))[0].astype(jnp.bfloat16)


def block_grads(x_blk, dy_blk, w_up, w_down):
    z_one = matmul(x_blk, w_up[0]).astype(jnp.bfloat16)
    act_one = gelu_fwd(z_one)
    hid_two = matmul(act_one, w_down[0]).astype(jnp.bfloat16)
    z_two = matmul(hid_two, w_up[1]).astype(jnp.bfloat16)
    act_two = gelu_fwd(z_two)
    grad_w4 = matmul(act_two.T, dy_blk)
    dact_two = matmul(dy_blk, w_down[1].T).astype(jnp.bfloat16)
    dz_two = gelu_back(z_two, dact_two)
    grad_w3 = matmul(hid_two.T, dz_two)
    dhid_two = matmul(dz_two, w_up[1].T).astype(jnp.bfloat16)
    grad_w2 = matmul(act_one.T, dhid_two)
    dact_one = matmul(dhid_two, w_down[0].T).astype(jnp.bfloat16)
    dz_one = gelu_back(z_one, dact_one)
    grad_w1 = matmul(x_blk.T, dz_one)
    return jnp.stack([grad_w1, grad_w3]), jnp.stack([grad_w2, grad_w4])


def adam_update(master_arr, mom_arr, var_arr, grad_arr, clip_scale, lr_val):
    scaled = clip_scale * grad_arr
    new_mom = BETA_ONE * mom_arr + (1.0 - BETA_ONE) * scaled
    new_var = BETA_TWO * var_arr + (1.0 - BETA_TWO) * scaled * scaled
    mom_hat = new_mom / (1.0 - BETA_ONE ** STEP)
    var_hat = new_var / (1.0 - BETA_TWO ** STEP)
    new_master = master_arr - lr_val * mom_hat / (jnp.sqrt(var_hat) + ADAM_EPS)
    return new_master, new_mom, new_var


def setup_inputs(seed: int = 0) -> dict:
    key_list = jax.random.split(jax.random.key(seed), 10)
    w_scale = D ** -0.5
    master_up = jax.random.normal(key_list[0], (2, D, FF), jnp.float32) * w_scale
    master_down = jax.random.normal(key_list[1], (2, FF, D), jnp.float32) * w_scale
    w_up = master_up.astype(jnp.bfloat16)
    w_down = master_down.astype(jnp.bfloat16)
    act_in = jax.random.normal(key_list[2], (ROWS, D), jnp.float32).astype(jnp.bfloat16)
    grad_out = jax.random.normal(key_list[3], (ROWS, D), jnp.float32).astype(jnp.bfloat16)
    est_up, est_down = block_grads(act_in[:TOKENS_DEV], grad_out[:TOKENS_DEV], w_up, w_down)
    sq_up = jnp.sum(est_up * est_up, axis=(1, 2)) / DATA
    sq_down = jnp.sum(est_down * est_down, axis=(1, 2)) / DATA
    est_norm = jnp.sqrt(jnp.sum(sq_up) + jnp.sum(sq_down))
    clip_frac = jax.random.uniform(key_list[4], (1,), jnp.float32, 0.3, 0.6)
    clip_norm = clip_frac * est_norm
    rms_up = clip_frac * jnp.sqrt(sq_up / (D * FF))
    rms_down = clip_frac * jnp.sqrt(sq_down / (D * FF))
    mom_up = jax.random.normal(key_list[5], (2, D, FF), jnp.float32) * rms_up[:, None, None]
    mom_down = jax.random.normal(key_list[6], (2, FF, D), jnp.float32) * rms_down[:, None, None]
    var_up = jax.random.uniform(key_list[7], (2, D, FF), jnp.float32, 0.25, 2.0) * (rms_up * rms_up)[:, None, None]
    var_down = jax.random.uniform(key_list[8], (2, FF, D), jnp.float32, 0.25, 2.0) * (rms_down * rms_down)[:, None, None]
    learn_rate = jax.random.uniform(key_list[9], (1,), jnp.float32, 0.1, 0.25) * w_scale
    return {"act_in": act_in, "grad_out": grad_out, "w_up": w_up, "w_down": w_down, "master_up": master_up, "master_down": master_down, "mom_up": mom_up, "mom_down": mom_down, "var_up": var_up, "var_down": var_down, "learn_rate": learn_rate, "clip_norm": clip_norm}


def reference(act_in, grad_out, w_up, w_down, master_up, master_down, mom_up, mom_down, var_up, var_down, learn_rate, clip_norm):
    x_blocks = act_in.reshape(DATA, TOKENS_DEV, D)
    dy_blocks = grad_out.reshape(DATA, TOKENS_DEV, D)

    def body_fn(carry_sum, block_pair):
        part_up, part_down = block_grads(block_pair[0], block_pair[1], w_up, w_down)
        return (carry_sum[0] + part_up, carry_sum[1] + part_down), None

    zero_sums = (jnp.zeros((2, D, FF), jnp.float32), jnp.zeros((2, FF, D), jnp.float32))
    grad_sums, _ = lax.scan(body_fn, zero_sums, (x_blocks, dy_blocks))
    grad_up = grad_sums[0] / DATA
    grad_down = grad_sums[1] / DATA
    sq_total = jnp.sum(grad_up * grad_up) + jnp.sum(grad_down * grad_down)
    norm_val = jnp.sqrt(sq_total)
    clip_scale = jnp.minimum(1.0, clip_norm[0] / (norm_val + NORM_EPS))
    lr_val = learn_rate[0]
    new_master_up, new_mom_up, new_var_up = adam_update(master_up, mom_up, var_up, grad_up, clip_scale, lr_val)
    new_master_down, new_mom_down, new_var_down = adam_update(master_down, mom_down, var_down, grad_down, clip_scale, lr_val)
    return (new_master_up.astype(jnp.bfloat16), new_master_down.astype(jnp.bfloat16), new_master_up, new_master_down, new_mom_up, new_mom_down, new_var_up, new_var_down, norm_val.reshape(1))
```

```python
import functools

import jax
import jax.numpy as jnp
from jax import lax
from jax.experimental import pallas as pl
from jax.experimental.pallas import tpu as pltpu
from jax.sharding import PartitionSpec as P

STEP = 10
BETA_ONE = 0.9
BETA_TWO = 0.95
ADAM_EPS = 1e-8
NORM_EPS = 1e-6
GELU_A = 0.7978845608028654
GELU_B = GELU_A * 0.044715
BF16 = jnp.bfloat16
F32 = jnp.float32
DOT_NT = (((1,), (1,)), ((), ()))
DOT_TN = (((0,), (0,)), ((), ()))
VMEM_LIMIT = 60 * 2**20


def gelu(z):
    half = 0.5 * z
    return half + half * jnp.tanh(z * (z * z * GELU_B + GELU_A))


def gelu_grad(z):
    sq = z * z
    sig = 0.5 * jnp.tanh(z * (sq * GELU_B + GELU_A)) + 0.5
    return sig + z * (sq * (6.0 * GELU_B) + 2.0 * GELU_A) * (sig - sig * sig)


def gelu_both(z):
    sq = z * z
    sig = 0.5 * jnp.tanh(z * (sq * GELU_B + GELU_A)) + 0.5
    act = z * sig
    return act, sig + (act - act * sig) * (sq * (6.0 * GELU_B) + 2.0 * GELU_A)


def col_chunks(width, step):
    return [slice(lo, min(lo + step, width)) for lo in range(0, width, step)]


def forward_body(x_ref, dy_ref, w1_ref, w2_ref, w3_ref, w4_ref, z1_ref, h_ref, a3_ref, q3_ref, a1_scr):
    x = x_ref[...]
    for cols in col_chunks(w1_ref.shape[1], 256):
        z = jnp.dot(x, w1_ref[:, cols], preferred_element_type=F32).astype(BF16)
        z1_ref[:, cols] = z
        a1_scr[:, cols] = gelu(z.astype(F32)).astype(BF16)
    h = jnp.dot(a1_scr[...], w2_ref[...], preferred_element_type=F32).astype(BF16)
    h_ref[...] = h
    dy = dy_ref[...]
    for cols in col_chunks(w3_ref.shape[1], 256):
        z = jnp.dot(h, w3_ref[:, cols], preferred_element_type=F32).astype(BF16)
        e = lax.dot_general(dy, w4_ref[cols, :], DOT_NT, preferred_element_type=F32).astype(BF16)
        act, slope = gelu_both(z.astype(F32))
        a3_ref[:, cols] = act.astype(BF16)
        q3_ref[:, cols] = (e.astype(F32) * slope).astype(BF16)


def grad_body(left_ref, right_ref, out_ref, *, act):
    left = left_ref[...]
    if act:
        left = gelu(left.astype(F32)).astype(BF16)
    out_ref[...] = lax.dot_general(left, right_ref[...], DOT_TN, preferred_element_type=F32)


def resident(shape):
    return pl.BlockSpec(shape, lambda i: (0,) * len(shape), pipeline_mode=pl.Buffered(1))


def row_tile(rows, width):
    return pl.BlockSpec((rows, width), lambda i: (i, 0))


def params():
    return pltpu.CompilerParams(vmem_limit_bytes=VMEM_LIMIT)


def cost(flops, moved):
    return pl.CostEstimate(flops=flops, bytes_accessed=moved, transcendentals=0)


def forward(x, dy, w1, w2, w3, w4, tile=512):
    rows, d = x.shape
    f = w1.shape[1]
    wide, slim = jax.ShapeDtypeStruct((rows, f), BF16), jax.ShapeDtypeStruct((rows, d), BF16)
    return pl.pallas_call(
        forward_body,
        grid=(rows // tile,),
        in_specs=[row_tile(tile, d), row_tile(tile, d), resident((d, f)), resident((f, d)), resident((d, f)), resident((f, d))],
        out_specs=[row_tile(tile, f), row_tile(tile, d), row_tile(tile, f), row_tile(tile, f)],
        out_shape=[wide, slim, wide, wide],
        scratch_shapes=[pltpu.VMEM((tile, f), BF16)],
        compiler_params=params(),
        cost_estimate=cost(8 * rows * d * f, 6 * rows * f),
        name="forward",
    )(x, dy, w1, w2, w3, w4)


MESH = pl.DeviceIdType.MESH
TILE = 512
BLOCK = 256


class Lanes:
    def __init__(self):
        data = lax.axis_index("data")
        self.model = lax.axis_index("model")
        self.x, self.core = data // 2, data % 2
        self.mate = {"data": 2 * self.x + (1 - self.core)}
        self.over_x = {"data": 2 * (1 - self.x) + self.core}
        self.over_y = {"model": 1 - self.model}
        self.all = (self.mate, self.over_x, self.over_y)

    def shard(self, far, core):
        return 2 * ((self.x + far) % 2) + core


def greet(lanes):
    barrier = pltpu.get_barrier_semaphore()
    for peer in lanes.all:
        pl.semaphore_signal(barrier, inc=1, device_id=peer, device_id_type=MESH)
    pl.semaphore_wait(barrier, len(lanes.all))


class Reducer:
    def __init__(self, lanes, up, bufs, send, recv, scratch, local):
        self.lanes, self.up, self.send, self.recv, self.local = lanes, up, send, recv, local
        self.grad, self.mated, self.chip, self.from_y, self.from_x, self.part_a, self.part_b, self.last_x, self.last_y = bufs
        self.left, self.right, self.out = scratch
        self.rows = self.left.shape[0] // 2
        self.copies = {}

    def block(self, half, shard):
        if self.up:
            rows, width = 2 * self.rows, self.left.shape[1]
            return self.grad.at[pl.ds(shard * rows, rows), pl.ds(half * width, width)]
        rows = 2 * self.rows
        return self.grad.at[pl.ds(half * 4 * rows + shard * rows, rows), :]

    def remote(self, slot, src, dst, peer):
        copy = pltpu.make_async_remote_copy(src, dst, self.send.at[slot], self.recv.at[slot], device_id=peer, device_id_type=MESH)
        self.copies[slot] = copy
        return copy

    def mate_copies(self):
        lanes = self.lanes
        out = []
        for half in range(2):
            for far in range(2):
                shard = lanes.shard(far, 1 - lanes.core)
                out.append(self.remote(2 * half + far, self.block(half, shard), self.mated.at[half, far], lanes.mate))
        return out

    def first(self, half, far):
        lanes, rows = self.lanes, self.rows
        chip = self.chip.at[half, far]
        sends = []
        if half == 1:
            sends.append(self.remote(4 + far, chip.at[pl.ds(0, rows)], self.from_y.at[far], lanes.over_y))
        if far == 1:
            sends.append(self.remote(6 + half, chip.at[pl.ds(rows, rows)], self.from_x.at[half], lanes.over_x))
        return Job(self, self.block(half, lanes.shard(far, lanes.core)), self.mated.at[half, far], chip, 2 * rows, (2 * half + far,), sends)

    def second_a(self, far):
        dst = self.part_a.at[far]
        sends = [self.remote(8, dst, self.last_x, self.lanes.over_x)] if far == 1 else []
        return Job(self, self.chip.at[0, far].at[pl.ds(0, self.rows)], self.from_y.at[far], dst, self.rows, (4 + far,), sends)

    def second_b(self, half):
        dst = self.part_b.at[half]
        sends = [self.remote(9, dst, self.last_y, self.lanes.over_y)] if half == 1 else []
        return Job(self, self.chip.at[half, 0].at[pl.ds(self.rows, self.rows)], self.from_x.at[half], dst, self.rows, (6 + half,), sends)

    def firsts(self):
        return [self.first(1, 1), self.first(1, 0), self.first(0, 1), self.first(0, 0)]

    def seconds(self):
        return [self.second_a(1), self.second_b(1), self.second_a(0), self.second_b(0)]

    def finish(self):
        for slot in (8, 9):
            self.copies[slot].wait_recv()
        for slot in range(10):
            self.copies[slot].wait_send()


class Job:
    def __init__(self, owner, left, right, dst, rows, arrivals, sends):
        view = lambda ref: ref.at[pl.ds(0, rows)]
        self.owner, self.arrivals, self.sends = owner, arrivals, sends
        self.bufs = view(owner.left), view(owner.right), view(owner.out)
        self.loads = [pltpu.make_async_copy(src, buf, owner.local.at[k]) for k, (src, buf) in enumerate(zip((left, right), self.bufs))]
        self.store = pltpu.make_async_copy(self.bufs[2], dst, owner.local.at[2])

    def start(self):
        for slot in self.arrivals:
            self.owner.copies[slot].wait_recv()
        for load in self.loads:
            load.start()

    def add(self):
        for load in self.loads:
            load.wait()
        left, right, out = self.bufs
        out[...] = left[...] + right[...]
        self.store.start()

    def done(self):
        self.store.wait()
        for copy in self.sends:
            copy.start()


class Plan:
    def __init__(self):
        self.pending = None

    def arrange(self, jobs):
        chain = []
        for at in sorted(jobs):
            chain.append((at, self.pending, jobs[at]))
            self.pending = jobs[at]
        return chain

    @staticmethod
    def beside(step, chain, work):
        for at, old, job in chain:
            @pl.when(step == at)
            def _(old=old, job=job):
                if old is not None:
                    old.done()
                job.start()
        work()
        for at, old, job in chain:
            @pl.when(step == at)
            def _(job=job):
                job.add()

    def run(self, jobs):
        for job in jobs:
            if self.pending is not None:
                self.pending.done()
            job.start()
            job.add()
            self.pending = job

    def flush(self):
        if self.pending is not None:
            self.pending.done()
        self.pending = None


def reduce_kernel(a3, q3, z1, h, x, dy, w3, w2, *refs):
    outs, scratch = refs[:37], refs[37:]
    q1 = outs[0]
    bufs = [outs[1 + 9 * k:10 + 9 * k] for k in range(4)]
    res0, res1, w3_v, w2_v, up_l, up_r, up_o, dn_l, dn_r, dn_o, send, recv, local, fetch = scratch
    lanes = Lanes()
    greet(lanes)
    reds = [Reducer(lanes, up, bufs[k], send.at[k], recv.at[k], (up_l, up_r, up_o) if up else (dn_l, dn_r, dn_o), local)
            for k, up in enumerate((False, True, False, True))]
    down4, up3, down2, up1 = reds
    load = lambda src, dst, k: pltpu.make_async_copy(src, dst, fetch.at[k])
    get_dy, get_h, get_x, get_w3, get_w2 = load(dy, res0, 0), load(h, res1, 1), load(x, res1, 2), load(w3, w3_v, 3), load(w2, w2_v, 4)
    rows, d = x.shape
    f = a3.shape[1]
    plan = Plan()

    def down_phase(left, right, grad, jobs, act):
        chain = plan.arrange(jobs)

        def body(ids, left_ref, out_ref):
            plan.beside(ids.index[0], chain, lambda: grad_body(left_ref, right, out_ref, act=act))
        pltpu.emit_pipeline(body, grid=(f // BLOCK,), in_specs=[pl.BlockSpec((rows, BLOCK), lambda i: (0, i))],
                            out_specs=[pl.BlockSpec((BLOCK, d), lambda i: (i, 0))], _explicit_indices=True)(left, grad)

    def up_phase(left, right, grad, jobs):
        chain = plan.arrange(jobs)

        def body(ids, right_ref, out_ref):
            plan.beside(ids.index[0], chain, lambda: grad_body(left, right_ref, out_ref, act=False))
        pltpu.emit_pipeline(body, grid=(f // BLOCK,), in_specs=[pl.BlockSpec((rows, BLOCK), lambda i: (0, i))],
                            out_specs=[pl.BlockSpec((d, BLOCK), lambda i: (0, i))], _explicit_indices=True)(right, grad)

    def e2_phase(jobs):
        chain = plan.arrange(jobs)

        def body(ids, q_ref):
            def work():
                e2 = lax.dot_general(q_ref[...], w3_v[...], DOT_NT, preferred_element_type=F32)
                res0[pl.ds(pl.multiple_of(ids.index[0] * TILE, TILE), TILE), :] = e2.astype(BF16)
            plan.beside(ids.index[0], chain, work)
        pltpu.emit_pipeline(body, grid=(rows // TILE,), in_specs=[pl.BlockSpec((TILE, f), lambda i: (i, 0))], _explicit_indices=True)(q3)

    def q1_phase(jobs):
        chain = plan.arrange(jobs)

        def body(ids, z_ref, q_ref):
            def work():
                e2 = res0[pl.ds(pl.multiple_of(ids.index[0] * TILE, TILE), TILE), :]
                for cols in col_chunks(f, 256):
                    e = lax.dot_general(e2, w2_v[cols, :], DOT_NT, preferred_element_type=F32).astype(BF16)
                    q_ref[:, cols] = (e.astype(F32) * gelu_grad(z_ref[:, cols].astype(F32))).astype(BF16)
            plan.beside(ids.index[0], chain, work)
        pltpu.emit_pipeline(body, grid=(rows // TILE,), in_specs=[pl.BlockSpec((TILE, f), lambda i: (i, 0))],
                            out_specs=[pl.BlockSpec((TILE, f), lambda i: (i, 0))], _explicit_indices=True)(z1, q1)

    def leave(red):
        for copy in red.mate_copies():
            copy.start()

    get_dy.start()
    get_dy.wait()
    get_h.start()
    get_w3.start()
    get_w2.start()
    down_phase(a3, res0, down4.grad, {}, False)
    leave(down4)
    get_h.wait()
    first4 = down4.firsts()
    up_phase(res1, q3, up3.grad, dict(zip((5, 6, 7, 8), first4)))
    leave(up3)
    get_x.start()
    get_w3.wait()
    first3 = up3.firsts()
    e2_phase(dict(zip((3, 4, 5, 6), first3)))
    second4 = down4.seconds()
    down_phase(z1, res0, down2.grad, dict(zip((1, 2, 3, 4), second4)), True)
    leave(down2)
    get_w2.wait()
    first2 = down2.firsts()
    second3 = up3.seconds()
    q1_phase(dict(zip((3, 4, 5, 6, 7), first2 + second3[:1])))
    get_x.wait()
    up_phase(res1, q1, up1.grad, dict(zip((0, 1, 2), second3[1:])))
    leave(up1)
    plan.run(down2.seconds())
    plan.run(up1.firsts())
    plan.run(up1.seconds())
    plan.flush()
    for red in reds:
        red.finish()


def reduce_gradients(a3, q3, z1, h, x, dy, w3, w2):
    rows, f = a3.shape
    d = x.shape[1]
    shapes = [jax.ShapeDtypeStruct((rows, f), BF16)]
    for up in (False, True, False, True):
        whole, width = ((d, f), f // 2) if up else ((f, d), d)
        part = (d if up else f // 2) // 4
        half = part // 2
        for shape in (whole, (2, 2, part, width), (2, 2, part, width), (2, half, width), (2, half, width),
                      (2, half, width), (2, half, width), (half, width), (half, width)):
            shapes.append(jax.ShapeDtypeStruct(shape, F32))
    up_block, down_block = pltpu.VMEM((d // 4, f // 2), F32), pltpu.VMEM((f // 8, d), F32)
    outs = pl.pallas_call(
        reduce_kernel,
        in_specs=[pl.BlockSpec(memory_space=pl.ANY)] * 8,
        out_specs=[pl.BlockSpec(memory_space=pl.ANY)] * len(shapes),
        out_shape=shapes,
        scratch_shapes=[
            pltpu.VMEM((rows, d), BF16), pltpu.VMEM((rows, d), BF16), pltpu.VMEM((d, f), BF16), pltpu.VMEM((f, d), BF16),
            up_block, up_block, up_block, down_block, down_block, down_block,
            pltpu.SemaphoreType.DMA((4, 10)), pltpu.SemaphoreType.DMA((4, 10)), pltpu.SemaphoreType.DMA((3,)), pltpu.SemaphoreType.DMA((5,)),
        ],
        compiler_params=pltpu.CompilerParams(vmem_limit_bytes=VMEM_LIMIT, collective_id=1, has_side_effects=True),
        cost_estimate=cost(12 * rows * d * f, 12 * rows * f),
        name="reduce_gradients",
    )(a3, q3, z1, h, x, dy, w3, w2)

    def shard(k):
        part_a, part_b, last_x, last_y = outs[1 + 9 * k + 5:10 + 9 * k]
        return jnp.concatenate([part_a[0] + last_x, part_b[0] + last_y], axis=0)

    return [shard(k) for k in range(4)]


def adam_update(master_arr, mom_arr, var_arr, grad_arr, clip_scale, lr_val):
    scaled = clip_scale * grad_arr
    new_mom = BETA_ONE * mom_arr + (1.0 - BETA_ONE) * scaled
    new_var = BETA_TWO * var_arr + (1.0 - BETA_TWO) * scaled * scaled
    mom_hat = new_mom / (1.0 - BETA_ONE ** STEP)
    var_hat = new_var / (1.0 - BETA_TWO ** STEP)
    new_master = master_arr - lr_val * mom_hat / (jnp.sqrt(var_hat) + ADAM_EPS)
    return new_master, new_mom, new_var


def solution(mesh):
    data_size = mesh.shape["data"]
    spec_rows = P("data", None)
    spec_wup = P(None, None, "model")
    spec_wdown = P(None, "model", None)
    spec_sup = P(None, "data", "model")
    spec_sdown = P(None, ("model", "data"), None)
    spec_scalar = P(None)

    def whole(own, dim):
        quarter = own.shape[1] // data_size
        mine = lax.dynamic_slice_in_dim(own, lax.axis_index("data") * quarter, quarter, 1)
        theirs = lax.ppermute(mine, "model", [(0, 1), (1, 0)])
        other = lax.all_gather(theirs, "data", axis=1, tiled=True)
        return jnp.concatenate([own, other], axis=dim)

    def local_step(act_in, grad_out, w_up, w_down, master_up, master_down, mom_up, mom_down, var_up, var_down, learn_rate, clip_norm):
        rows = act_in.shape[0] // 2
        start = lax.axis_index("model") * rows
        x = lax.dynamic_slice_in_dim(act_in, start, rows, 0)
        dy = lax.dynamic_slice_in_dim(grad_out, start, rows, 0)
        up, down = whole(w_up, 2), whole(w_down, 1)
        z1, h, a3, q3 = forward(x, dy, up[0], down[0], up[1], down[1])
        shard_w4, shard_w3, shard_w2, shard_w1 = reduce_gradients(a3, q3, z1, h, x, dy, up[1], down[0])
        grad_up_arr = jnp.stack([shard_w1, shard_w3]) / data_size
        grad_down_arr = jnp.stack([shard_w2, shard_w4]) / data_size
        sq_local = jnp.sum(grad_up_arr * grad_up_arr) + jnp.sum(grad_down_arr * grad_down_arr)
        norm_val = jnp.sqrt(lax.psum(sq_local, ("model", "data")))
        clip_scale = jnp.minimum(1.0, clip_norm[0] / (norm_val + NORM_EPS))
        lr_val = learn_rate[0]
        new_master_up, new_mom_up, new_var_up = adam_update(master_up, mom_up, var_up, grad_up_arr, clip_scale, lr_val)
        new_master_down, new_mom_down, new_var_down = adam_update(master_down, mom_down, var_down, grad_down_arr, clip_scale, lr_val)
        new_w_up = lax.all_gather(new_master_up.astype(BF16), "data", axis=1, tiled=True)
        new_w_down = lax.all_gather(new_master_down.astype(BF16), "data", axis=1, tiled=True)
        return (new_w_up, new_w_down, new_master_up, new_master_down, new_mom_up, new_mom_down, new_var_up, new_var_down, norm_val.reshape(1))

    return jax.shard_map(local_step, mesh=mesh, in_specs=(spec_rows, spec_rows, spec_wup, spec_wdown, spec_sup, spec_sdown, spec_sup, spec_sdown, spec_sup, spec_sdown, spec_scalar, spec_scalar), out_specs=(spec_wup, spec_wdown, spec_sup, spec_sdown, spec_sup, spec_sdown, spec_sup, spec_sdown, spec_scalar), check_vma=False)
```

```python
import functools

import jax
import jax.numpy as jnp
from jax import lax
from jax.experimental import pallas as pl
from jax.experimental.pallas import tpu as pltpu
from jax.sharding import PartitionSpec as P

STEP = 10
BETA_ONE = 0.9
BETA_TWO = 0.95
ADAM_EPS = 1e-8
NORM_EPS = 1e-6
GELU_A = 0.7978845608028654
GELU_B = GELU_A * 0.044715
BF16 = jnp.bfloat16
F32 = jnp.float32
DOT_NT = (((1,), (1,)), ((), ()))
DOT_TN = (((0,), (0,)), ((), ()))
VMEM_LIMIT = 60 * 2**20


def gelu(z):
    half = 0.5 * z
    return half + half * jnp.tanh(z * (z * z * GELU_B + GELU_A))


def gelu_grad(z):
    sq = z * z
    sig = 0.5 * jnp.tanh(z * (sq * GELU_B + GELU_A)) + 0.5
    return sig + z * (sq * (6.0 * GELU_B) + 2.0 * GELU_A) * (sig - sig * sig)


def gelu_both(z):
    sq = z * z
    sig = 0.5 * jnp.tanh(z * (sq * GELU_B + GELU_A)) + 0.5
    act = z * sig
    return act, sig + (act - act * sig) * (sq * (6.0 * GELU_B) + 2.0 * GELU_A)


def col_chunks(width, step):
    return [slice(lo, min(lo + step, width)) for lo in range(0, width, step)]


def grad_body(left_ref, right_ref, out_ref, *, act):
    left = left_ref[...]
    if act:
        left = gelu(left.astype(F32)).astype(BF16)
    out_ref[...] = lax.dot_general(left, right_ref[...], DOT_TN, preferred_element_type=F32)


def cost(flops, moved):
    return pl.CostEstimate(flops=flops, bytes_accessed=moved, transcendentals=0)


MESH = pl.DeviceIdType.MESH
TILE = 512
BLOCK = 256


class Lanes:
    def __init__(self):
        data = lax.axis_index("data")
        self.model = lax.axis_index("model")
        self.x, self.core = data // 2, data % 2
        self.mate = {"data": 2 * self.x + (1 - self.core)}
        self.over_x = {"data": 2 * (1 - self.x) + self.core}
        self.over_y = {"model": 1 - self.model}
        self.near = (self.mate, self.over_x, self.over_y)
        self.place = 4 * self.model + data

    def others(self):
        places = [(self.place + step) % 8 for step in range(1, 8)]
        return [{"model": place // 4, "data": place % 4} for place in places]

    def shard(self, far, core):
        return 2 * ((self.x + far) % 2) + core


def greet(peers):
    barrier = pltpu.get_barrier_semaphore()
    for peer in peers:
        pl.semaphore_signal(barrier, inc=1, device_id=peer, device_id_type=MESH)
    pl.semaphore_wait(barrier, len(peers))


class Gather:
    def __init__(self, lanes, own, whole, up, send, recv):
        self.send, self.recv = send, recv
        data = lanes.shard(0, lanes.core)
        half = own.shape[1] if up else own.shape[0]
        part = own.shape[0] // 4

        def quarter(shard):
            if up:
                return whole.at[pl.ds(shard * part, part), pl.ds(half, half)]
            return whole.at[pl.ds(half + shard * part, part), :]

        near, far = quarter(data), quarter(lanes.shard(1, lanes.core))
        self.over_y = self.remote(0, own.at[pl.ds(data * part, part), :], near, lanes.over_y)
        self.over_x = self.remote(1, near, near, lanes.over_x)
        self.near = self.remote(2, near, near, lanes.mate)
        self.far = self.remote(3, far, far, lanes.mate)

    def remote(self, slot, src, dst, peer):
        return pltpu.make_async_remote_copy(src, dst, self.send.at[slot], self.recv.at[slot], device_id=peer, device_id_type=MESH)

    def start(self):
        self.over_y.start()

    def pass_near(self):
        self.over_y.wait_recv()
        self.over_x.start()
        self.near.start()

    def pass_far(self):
        self.over_x.wait_recv()
        self.far.start()

    def arrived(self):
        self.near.wait_recv()
        self.far.wait_recv()

    def sent(self):
        for copy in (self.over_y, self.over_x, self.near, self.far):
            copy.wait_send()


def at_steps(step, events):
    for at, event in events.items():
        @pl.when(step == at)
        def _(event=event):
            event()


def forward_kernel(act, grad, w_up, w_down, z1, h, a3, q3, e3, w3_out, w2_out, w1_v, w2_v, w3_v, w4_v, a1_v, send, recv, fetch):
    lanes = Lanes()
    greet(lanes.near)
    owns = [(w_up.at[0], w1_v, True), (w_down.at[0], w2_v, False), (w_up.at[1], w3_v, True), (w_down.at[1], w4_v, False)]
    gathers = [Gather(lanes, own, whole, up, send.at[k], recv.at[k]) for k, (own, whole, up) in enumerate(owns)]
    g1, g2, g3, g4 = gathers
    for gather in gathers:
        gather.start()
    half = w_up.shape[2]
    loads = []
    for k, (own, whole, up) in enumerate(owns):
        place = whole.at[:, pl.ds(0, half)] if up else whole.at[pl.ds(0, half), :]
        loads.append(pltpu.make_async_copy(own, place, fetch.at[k]))
    for k in (0, 3, 1, 2):
        loads[k].start()
    rows, d = h.shape
    f = z1.shape[1]
    steps = rows // TILE
    first = lanes.model * steps
    mine = pl.BlockSpec((TILE, d), lambda i: (first + i, 0))
    slim = pl.BlockSpec((TILE, d), lambda i: (i, 0))
    wide = pl.BlockSpec((TILE, f), lambda i: (i, 0))
    left = pl.BlockSpec((TILE, half), lambda i: (i, 0))
    right = pl.BlockSpec((TILE, half), lambda i: (i, 1))

    def own_body(ids, x_ref, dy_ref, z_ref, e_ref):
        at_steps(ids.index[0], {5: g1.pass_near})
        z_ref[...] = jnp.dot(x_ref[...], w1_v[:, :half], preferred_element_type=F32).astype(BF16)
        e_ref[...] = lax.dot_general(dy_ref[...], w4_v[:half, :], DOT_NT, preferred_element_type=F32).astype(BF16)

    def other_body(ids, x_ref, z_ref):
        def pass_on():
            g2.pass_far()
            g3.pass_near()

        at_steps(ids.index[0], {7: pass_on})
        z_ref[...] = jnp.dot(x_ref[...], w1_v[:, half:], preferred_element_type=F32).astype(BF16)

    def h_body(ids, z_ref, h_ref):
        def pass_on():
            g4.pass_near()
            g3.pass_far()

        at_steps(ids.index[0], {4: pass_on})
        for cols in col_chunks(f, 256):
            a1_v[:, cols] = gelu(z_ref[:, cols].astype(F32)).astype(BF16)
        h_ref[...] = jnp.dot(a1_v[...], w2_v[...], preferred_element_type=F32).astype(BF16)

    def last_body(ids, h_ref, dy_ref, e_ref, a_ref, q_ref):
        hid, dy = h_ref[...], dy_ref[...]
        for lo, hi in halves(half):
            cols = slice(lo, hi)
            z = jnp.dot(hid, w3_v[:, cols], preferred_element_type=F32).astype(BF16)
            if hi <= half:
                e = e_ref[:, cols]
            else:
                e = lax.dot_general(dy, w4_v[cols, :], DOT_NT, preferred_element_type=F32).astype(BF16)
            act_val, slope = gelu_both(z.astype(F32))
            a_ref[:, cols] = act_val.astype(BF16)
            q_ref[:, cols] = (e.astype(F32) * slope).astype(BF16)

    def pipe(body, ins, outs, refs):
        pltpu.emit_pipeline(body, grid=(steps,), in_specs=ins, out_specs=outs, _explicit_indices=True)(*refs)

    loads[0].wait()
    loads[3].wait()
    pipe(own_body, [mine, mine], [left, left], (act, grad, z1, e3))
    loads[1].wait()
    loads[2].wait()
    g2.pass_near()
    g1.pass_far()
    g1.arrived()
    pipe(other_body, [mine], [right], (act, z1))
    g2.arrived()
    save2 = pltpu.make_async_copy(w2_v, w2_out, fetch.at[0])
    save2.start()
    pipe(h_body, [wide], [slim], (z1, h))
    g4.pass_far()
    g3.arrived()
    g4.arrived()
    save3 = pltpu.make_async_copy(w3_v, w3_out, fetch.at[1])
    save3.start()
    pipe(last_body, [slim, mine, left], [wide, wide], (h, grad, e3, a3, q3))
    save2.wait()
    save3.wait()
    for gather in gathers:
        gather.sent()


def halves(half):
    return [(base + cols.start, base + cols.stop) for base in (0, half) for cols in col_chunks(half, 256)]


def forward(act, grad, w_up, w_down):
    d, half = w_up.shape[1:]
    rows, f = act.shape[0] // 2, 2 * half
    wide, slim, own = (jax.ShapeDtypeStruct((rows, n), BF16) for n in (f, d, half))
    up, down = (d, f), (f, d)
    outs = [wide, slim, wide, wide, own, jax.ShapeDtypeStruct(up, BF16), jax.ShapeDtypeStruct(down, BF16)]
    z1, h, a3, q3, _, w3, w2 = pl.pallas_call(
        forward_kernel,
        in_specs=[pl.BlockSpec(memory_space=pl.ANY)] * 4,
        out_specs=[pl.BlockSpec(memory_space=pl.ANY)] * len(outs),
        out_shape=outs,
        scratch_shapes=[pltpu.VMEM(up, BF16), pltpu.VMEM(down, BF16), pltpu.VMEM(up, BF16), pltpu.VMEM(down, BF16), pltpu.VMEM((TILE, f), BF16),
                        pltpu.SemaphoreType.DMA((4, 4)), pltpu.SemaphoreType.DMA((4, 4)), pltpu.SemaphoreType.DMA((4,))],
        compiler_params=pltpu.CompilerParams(vmem_limit_bytes=VMEM_LIMIT, collective_id=0, has_side_effects=True),
        cost_estimate=cost(8 * rows * d * f, 8 * rows * f),
        name="forward",
    )(act, grad, w_up, w_down)
    return z1, h, a3, q3, w3, w2


class Reducer:
    def __init__(self, lanes, up, bufs, send, recv, scratch, local, squares):
        self.lanes, self.up, self.send, self.recv, self.local = lanes, up, send, recv, local
        self.squares = squares
        self.grad, self.mated, self.chip, self.from_y, self.from_x, self.part_a, self.part_b, self.last_x, self.last_y, self.shard = bufs
        self.left, self.right, self.out = scratch
        self.rows = self.left.shape[0] // 2
        self.copies = {}
        for half in range(2):
            self.leave(half)

    def block(self, half, shard):
        if self.up:
            rows, width = 2 * self.rows, self.left.shape[1]
            return self.grad.at[pl.ds(shard * rows, rows), pl.ds(half * width, width)]
        rows = 2 * self.rows
        return self.grad.at[pl.ds(half * 4 * rows + shard * rows, rows), :]

    def remote(self, slot, src, dst, peer):
        copy = pltpu.make_async_remote_copy(src, dst, self.send.at[slot], self.recv.at[slot], device_id=peer, device_id_type=MESH)
        self.copies[slot] = copy
        return copy

    def leave(self, half):
        lanes = self.lanes
        for far in range(2):
            shard = lanes.shard(far, 1 - lanes.core)
            self.remote(2 * half + far, self.block(half, shard), self.mated.at[half, far], lanes.mate)

    def go(self, half):
        for far in range(2):
            self.copies[2 * half + far].start()

    def first(self, half, far):
        lanes, rows = self.lanes, self.rows
        chip = self.chip.at[half, far]
        sends = []
        if half == 1:
            sends.append(self.remote(4 + far, chip.at[pl.ds(0, rows)], self.from_y.at[far], lanes.over_y))
        if far == 1:
            sends.append(self.remote(6 + half, chip.at[pl.ds(rows, rows)], self.from_x.at[half], lanes.over_x))
        return Job(self, self.block(half, lanes.shard(far, lanes.core)), self.mated.at[half, far], chip, 2 * rows, (2 * half + far,), sends)

    def second_a(self, far):
        dst = self.part_a.at[far]
        sends = [self.remote(8, dst, self.last_x, self.lanes.over_x)] if far == 1 else []
        return Job(self, self.chip.at[0, far].at[pl.ds(0, self.rows)], self.from_y.at[far], dst, self.rows, (4 + far,), sends)

    def second_b(self, half):
        dst = self.part_b.at[half]
        sends = [self.remote(9, dst, self.last_y, self.lanes.over_y)] if half == 1 else []
        return Job(self, self.chip.at[half, 0].at[pl.ds(self.rows, self.rows)], self.from_x.at[half], dst, self.rows, (6 + half,), sends)

    def thirds(self):
        top, bottom = self.shard.at[pl.ds(0, self.rows)], self.shard.at[pl.ds(self.rows, self.rows)]
        return [Job(self, self.part_a.at[0], self.last_x, top, self.rows, (8,), [], True),
                Job(self, self.part_b.at[0], self.last_y, bottom, self.rows, (9,), [], True)]

    def firsts(self):
        return [self.first(1, 1), self.first(1, 0), self.first(0, 1), self.first(0, 0)]

    def seconds(self):
        return [self.second_a(1), self.second_b(1), self.second_a(0), self.second_b(0)]

    def finish(self):
        for slot in range(10):
            self.copies[slot].wait_send()


class Job:
    def __init__(self, owner, left, right, dst, rows, arrivals, sends, last=False):
        view = lambda ref: ref.at[pl.ds(0, rows)]
        self.owner, self.arrivals, self.sends, self.last = owner, arrivals, sends, last
        self.bufs = view(owner.left), view(owner.right), view(owner.out)
        self.loads = [pltpu.make_async_copy(src, buf, owner.local.at[k]) for k, (src, buf) in enumerate(zip((left, right), self.bufs))]
        self.store = pltpu.make_async_copy(self.bufs[2], dst, owner.local.at[2])

    def start(self):
        for slot in self.arrivals:
            self.owner.copies[slot].wait_recv()
        for load in self.loads:
            load.start()

    def add(self):
        for load in self.loads:
            load.wait()
        left, right, out = self.bufs
        if self.last:
            value = (left[...] + right[...]) * 0.25
            out[...] = value
            self.owner.squares[...] += jnp.sum((value * value).reshape(-1, 8, value.shape[1]), axis=0)
        else:
            out[...] = left[...] + right[...]
        self.store.start()

    def done(self):
        self.store.wait()
        for copy in self.sends:
            copy.start()


class Plan:
    def __init__(self):
        self.pending = None

    def arrange(self, jobs):
        chain = []
        for at in sorted(jobs):
            chain.append((at, self.pending, jobs[at]))
            self.pending = jobs[at]
        return chain

    @staticmethod
    def beside(step, chain, work):
        for at, old, job in chain:
            @pl.when(step == at)
            def _(old=old, job=job):
                if old is not None:
                    old.done()
                job.start()
        work()
        for at, old, job in chain:
            @pl.when(step == at)
            def _(job=job):
                job.add()

    def run(self, jobs):
        for job in jobs:
            if self.pending is not None:
                self.pending.done()
            job.start()
            job.add()
            self.pending = job

    def flush(self):
        if self.pending is not None:
            self.pending.done()
        self.pending = None


def reduce_kernel(a3, q3, z1, h, act_in, grad_out, w3, w2, *refs):
    outs, scratch = refs[:42], refs[42:]
    q1, norm_out = outs[:2]
    bufs = [outs[2 + 10 * k:12 + 10 * k] for k in range(4)]
    res0, res1, w3_v, w2_v, up_l, up_r, up_o, dn_l, dn_r, dn_o, up_sq, dn_sq, mine_sq, all_sq, send, recv, local, fetch, sq_send, sq_recv = scratch
    lanes = Lanes()
    greet(lanes.others())
    reds = [Reducer(lanes, up, bufs[k], send.at[k], recv.at[k], (up_l, up_r, up_o) if up else (dn_l, dn_r, dn_o), local,
                    up_sq if up else dn_sq)
            for k, up in enumerate((False, True, False, True))]
    down4, up3, down2, up1 = reds
    rows, f = a3.shape
    d = h.shape[1]
    mine = pl.ds(lanes.model * rows, rows)
    x, dy = act_in.at[mine, :], grad_out.at[mine, :]
    load = lambda src, dst, k: pltpu.make_async_copy(src, dst, fetch.at[k])
    get_dy, get_h, get_x, get_w3, get_w2 = load(dy, res0, 0), load(h, res1, 1), load(x, res1, 2), load(w3, w3_v, 3), load(w2, w2_v, 4)
    plan = Plan()
    up_sq[...] = jnp.zeros_like(up_sq)
    dn_sq[...] = jnp.zeros_like(dn_sq)

    def down_phase(left, right, grad, jobs, act):
        chain = plan.arrange(jobs)

        def body(ids, left_ref, out_ref):
            plan.beside(ids.index[0], chain, lambda: grad_body(left_ref, right, out_ref, act=act))
        pltpu.emit_pipeline(body, grid=(f // BLOCK,), in_specs=[pl.BlockSpec((rows, BLOCK), lambda i: (0, i))],
                            out_specs=[pl.BlockSpec((BLOCK, d), lambda i: (i, 0))], _explicit_indices=True)(left, grad)

    def up_phase(left, right, grad, jobs, events=None, skip=0):
        chain, blocks = plan.arrange(jobs), f // BLOCK

        def body(ids, right_ref, out_ref):
            at_steps(ids.index[0], events or {})
            plan.beside(ids.index[0], chain, lambda: grad_body(left, right_ref, out_ref, act=False))
        place = lambda i: (0, (i + skip) % blocks)
        pltpu.emit_pipeline(body, grid=(blocks,), in_specs=[pl.BlockSpec((rows, BLOCK), place)],
                            out_specs=[pl.BlockSpec((d, BLOCK), place)], _explicit_indices=True)(right, grad)

    def e2_phase(jobs):
        chain = plan.arrange(jobs)

        def body(ids, q_ref):
            def work():
                e2 = lax.dot_general(q_ref[...], w3_v[...], DOT_NT, preferred_element_type=F32)
                res0[pl.ds(pl.multiple_of(ids.index[0] * TILE, TILE), TILE), :] = e2.astype(BF16)
            plan.beside(ids.index[0], chain, work)
        pltpu.emit_pipeline(body, grid=(rows // TILE,), in_specs=[pl.BlockSpec((TILE, f), lambda i: (i, 0))], _explicit_indices=True)(q3)

    def q1_phase(jobs):
        chain = plan.arrange(jobs)

        def body(ids, z_ref, q_ref):
            def work():
                e2 = res0[pl.ds(pl.multiple_of(ids.index[0] * TILE, TILE), TILE), :]
                for cols in col_chunks(f, 256):
                    e = lax.dot_general(e2, w2_v[cols, :], DOT_NT, preferred_element_type=F32).astype(BF16)
                    q_ref[:, cols] = (e.astype(F32) * gelu_grad(z_ref[:, cols].astype(F32))).astype(BF16)
            plan.beside(ids.index[0], chain, work)
        pltpu.emit_pipeline(body, grid=(rows // TILE,), in_specs=[pl.BlockSpec((TILE, f), lambda i: (i, 0))],
                            out_specs=[pl.BlockSpec((TILE, f), lambda i: (i, 0))], _explicit_indices=True)(z1, q1)

    def leave(red):
        red.go(0)
        red.go(1)

    get_dy.start()
    get_dy.wait()
    get_h.start()
    get_w3.start()
    get_w2.start()
    down_phase(a3, res0, down4.grad, {}, False)
    leave(down4)
    get_h.wait()
    first4 = down4.firsts()
    up_phase(res1, q3, up3.grad, dict(zip((5, 6, 7, 8), first4)))
    leave(up3)
    get_x.start()
    get_w3.wait()
    first3 = up3.firsts()
    e2_phase(dict(zip((3, 4, 5, 6), first3)))
    second4 = down4.seconds()
    down_phase(z1, res0, down2.grad, dict(zip((1, 2, 3, 4), second4)), True)
    leave(down2)
    get_w2.wait()
    first2 = down2.firsts()
    second3 = up3.seconds()
    q1_phase(dict(zip(range(8), second3[:2] + first2 + second3[2:])))
    get_x.wait()
    second2 = down2.seconds()
    first1 = up1.firsts()
    beside1 = down4.thirds() + up3.thirds() + second2 + first1[:1]
    up_phase(res1, q1, up1.grad, dict(zip((0, 1, 2, 3, 5, 6, 8, 9, 10), beside1)), {7: lambda: up1.go(1)}, f // 2 // BLOCK)
    up1.go(0)
    plan.run(first1[1:])
    plan.run(down2.thirds())
    plan.run(up1.seconds())
    plan.run(up1.thirds())
    plan.flush()
    total = dn_sq[:, :128] + up_sq[:, :128]
    for cols in col_chunks(d, 128)[1:]:
        total += dn_sq[:, cols]
    for cols in col_chunks(f // 2, 128)[1:]:
        total += up_sq[:, cols]
    mine_sq[...] = total
    copies = []
    for k, peer in enumerate(lanes.others()):
        copy = pltpu.make_async_remote_copy(mine_sq, all_sq.at[lanes.place], sq_send.at[k], sq_recv.at[k], device_id=peer, device_id_type=MESH)
        copy.start()
        copies.append(copy)
    own = pltpu.make_async_copy(mine_sq, all_sq.at[lanes.place], local.at[0])
    own.start()
    own.wait()
    for red in reds:
        red.finish()
    for copy in copies:
        copy.wait()
    norm_out[...] = jnp.sum(all_sq[...], axis=0)


def reduce_gradients(a3, q3, z1, h, act_in, grad_out, w3, w2):
    rows, f = a3.shape
    d = h.shape[1]
    shapes = [jax.ShapeDtypeStruct((rows, f), BF16), jax.ShapeDtypeStruct((8, 128), F32)]
    for up in (False, True, False, True):
        whole, width = ((d, f), f // 2) if up else ((f, d), d)
        part = (d if up else f // 2) // 4
        half = part // 2
        for shape in (whole, (2, 2, part, width), (2, 2, part, width), (2, half, width), (2, half, width),
                      (2, half, width), (2, half, width), (half, width), (half, width), (part, width)):
            shapes.append(jax.ShapeDtypeStruct(shape, F32))
    up_block, down_block = pltpu.VMEM((d // 4, f // 2), F32), pltpu.VMEM((f // 8, d), F32)
    outs = pl.pallas_call(
        reduce_kernel,
        in_specs=[pl.BlockSpec(memory_space=pl.ANY)] * 8,
        out_specs=[pl.BlockSpec(memory_space=pltpu.VMEM if k == 1 else pl.ANY) for k in range(len(shapes))],
        out_shape=shapes,
        scratch_shapes=[
            pltpu.VMEM((rows, d), BF16), pltpu.VMEM((rows, d), BF16), pltpu.VMEM((d, f), BF16), pltpu.VMEM((f, d), BF16),
            up_block, up_block, up_block, down_block, down_block, down_block,
            pltpu.VMEM((8, f // 2), F32), pltpu.VMEM((8, d), F32), pltpu.VMEM((8, 128), F32), pltpu.VMEM((8, 8, 128), F32),
            pltpu.SemaphoreType.DMA((4, 10)), pltpu.SemaphoreType.DMA((4, 10)), pltpu.SemaphoreType.DMA((3,)), pltpu.SemaphoreType.DMA((5,)),
            pltpu.SemaphoreType.DMA((7,)), pltpu.SemaphoreType.DMA((7,)),
        ],
        compiler_params=pltpu.CompilerParams(vmem_limit_bytes=VMEM_LIMIT, collective_id=1, has_side_effects=True),
        cost_estimate=cost(12 * rows * d * f, 12 * rows * f),
        name="reduce_gradients",
    )(a3, q3, z1, h, act_in, grad_out, w3, w2)

    return [outs[11 + 10 * k] for k in range(4)], jnp.sum(outs[1])


def adam_update(master_arr, mom_arr, var_arr, grad_arr, clip_scale, lr_val):
    scaled = clip_scale * grad_arr
    new_mom = BETA_ONE * mom_arr + (1.0 - BETA_ONE) * scaled
    new_var = BETA_TWO * var_arr + (1.0 - BETA_TWO) * scaled * scaled
    mom_hat = new_mom / (1.0 - BETA_ONE ** STEP)
    var_hat = new_var / (1.0 - BETA_TWO ** STEP)
    new_master = master_arr - lr_val * mom_hat / (jnp.sqrt(var_hat) + ADAM_EPS)
    return new_master, new_mom, new_var


def solution(mesh):
    data_size = mesh.shape["data"]
    spec_rows = P("data", None)
    spec_wup = P(None, None, "model")
    spec_wdown = P(None, "model", None)
    spec_sup = P(None, "data", "model")
    spec_sdown = P(None, ("model", "data"), None)
    spec_scalar = P(None)

    def spread(own):
        over_x, over_core = [(i, i ^ 2) for i in range(4)], [(i, i ^ 1) for i in range(4)]
        far = lax.ppermute(own, "data", over_x)
        mate = lax.ppermute(own, "data", over_core)
        far_mate = lax.ppermute(far, "data", over_core)
        data, part = lax.axis_index("data"), own.shape[1]
        out = jnp.broadcast_to(own[:1, :1, :1], (own.shape[0], data_size * part, own.shape[2]))
        for flip, rows in ((0, own), (1, mate), (2, far), (3, far_mate)):
            out = lax.dynamic_update_slice_in_dim(out, rows, (data ^ flip) * part, 1)
        return out

    def local_step(act_in, grad_out, w_up, w_down, master_up, master_down, mom_up, mom_down, var_up, var_down, learn_rate, clip_norm):
        z1, h, a3, q3, w3, w2 = forward(act_in, grad_out, w_up, w_down)
        (shard_w4, shard_w3, shard_w2, shard_w1), squares = reduce_gradients(a3, q3, z1, h, act_in, grad_out, w3, w2)
        grad_up_arr = jnp.stack([shard_w1, shard_w3])
        grad_down_arr = jnp.stack([shard_w2, shard_w4])
        norm_val = jnp.sqrt(squares)
        clip_scale = jnp.minimum(1.0, clip_norm[0] / (norm_val + NORM_EPS))
        lr_val = learn_rate[0]
        new_master_up, new_mom_up, new_var_up = adam_update(master_up, mom_up, var_up, grad_up_arr, clip_scale, lr_val)
        new_master_down, new_mom_down, new_var_down = adam_update(master_down, mom_down, var_down, grad_down_arr, clip_scale, lr_val)
        new_w_up, new_w_down = spread(new_master_up.astype(BF16)), spread(new_master_down.astype(BF16))
        return (new_w_up, new_w_down, new_master_up, new_master_down, new_mom_up, new_mom_down, new_var_up, new_var_down, norm_val.reshape(1))

    return jax.shard_map(local_step, mesh=mesh, in_specs=(spec_rows, spec_rows, spec_wup, spec_wdown, spec_sup, spec_sdown, spec_sup, spec_sdown, spec_sup, spec_sdown, spec_scalar, spec_scalar), out_specs=(spec_wup, spec_wdown, spec_sup, spec_sdown, spec_sup, spec_sdown, spec_sup, spec_sdown, spec_scalar), check_vma=False)
```
